32 devices in a mesh: row: 2 (over x), col: 16 (over z, y, core).
Axes of the slice: x: 2, y: 2, z: 4, core: 2. Of those that a mesh axis runs over, the one named last changes fastest.
Arguments:
- ld_matrix: bfloat16 [32768, 32768], P('row', 'col'), may hold values from -0.23925781 to 0.23925781
- factor: float32 [32768, 256], P(('row', 'col')), may hold values from -0.24 to 0.24
- diag_values: bfloat16 [32768], P('col'), may hold values from 0.5 to 4
Outputs:
- factor_grad: float32 [32768, 256], P(('row', 'col'))
The draws below stay inside these ranges and needn't reach their ends.
All inputs are finite; a program needn't handle non-finite values.
Results may differ from the reference program's by a relative error of at most 0.003.
Values may be sent and summed in bfloat16 or wider, within the bound.
A program may use at most 128 MiB of HBM per device.

```python
import math
import jax
import jax.numpy as jnp
from jax import lax

M = 32768
K = 256


def strengthened(values, stream_key, source, target, shards_of, factor):
    owner, partner = [(jnp.arange(values.shape[axis_at]) // (values.shape[axis_at] // shards_of)).reshape([-1 if axis == axis_at else 1 for axis in range(values.ndim)]) for axis_at in (source, target)]
    chosen = jax.random.permutation(stream_key, shards_of)[partner]
    strong = (owner == chosen) | (owner == (partner + shards_of // 2) % shards_of)
    return jnp.where(strong, factor * values, values)


def block_levels(rng, extent, split, smallest, high):
    def one(dim, parts):
        steps = jax.random.uniform(jax.random.fold_in(jax.random.fold_in(rng, 6), dim), (parts,), jnp.float32, smallest / len(split), high / len(split))
        return jnp.repeat(jnp.exp(steps), extent[dim] // parts).reshape((-1,) + (1,) * (len(extent) - dim - 1))

    level = one(*split[0])
    for cut in split[1:]:
        level = level * one(*cut)
    return level


def normal_values(stream_key, extent, deviation, reach, shards=(), kind=jnp.bfloat16):
    gain = block_levels(stream_key, extent, shards, -0.22, 0.18) if shards else 1.0
    entries = jax.random.normal(stream_key, extent, jnp.float32) * deviation * gain
    return jnp.minimum(jnp.maximum(entries, -reach), reach).astype(kind)


def heavy_noise(own_key, extent, width, most, split, heavy, held_as=jnp.bfloat16):
    drawn = width * jax.random.normal(own_key, extent, jnp.float32)
    if split:
        drawn = drawn * block_levels(own_key, extent, split, -0.22, 0.18)
    return jnp.clip(strengthened(drawn, jax.random.fold_in(own_key, 3), *heavy), -most, most).astype(held_as)


def setup_inputs(seed: int = 0) -> dict:
    key_list = jax.random.split(jax.random.key(seed), 4)
    return {
        "ld_matrix": heavy_noise(key_list[0], (M, M), 0.03, 0.23925781, ((0, 2), (1, 16)), (1, 0, 16, 2.0)),
        "factor": normal_values(key_list[1], (M, K), 0.03, 0.24, ((0, 32),), jnp.float32),
        "diag_values": jnp.clip(jnp.exp(math.log(4.0) - 2.0794415 * jax.random.uniform(key_list[2], (M,), jnp.float32) ** block_levels(key_list[2], (M,), ((0, 16),), -0.2, 0.2)), 0.5, 4.0).astype(jnp.bfloat16),
    }


def reference(ld_matrix, factor, diag_values):
    factor_low = factor.astype(jnp.bfloat16)
    height = min(1024, M)
    count = M // height
    ld_blocks = ld_matrix.reshape(count, height, M)
    diag_full = diag_values.astype(jnp.float32)
    columns = jnp.arange(M, dtype=jnp.int32)

    def one_block(inputs):
        index, ld_block = inputs
        start = (index * height).astype(jnp.int32)
        left = lax.dynamic_slice_in_dim(factor_low, start, height, 0)
        model_part = jnp.dot(left, factor_low.T, preferred_element_type=jnp.float32)
        row_ids = start + jnp.arange(height, dtype=jnp.int32)
        ondiag = row_ids[:, None] == columns[None, :]
        extra = jnp.where(ondiag, diag_full[None, :], jnp.float32(0.0))
        misfit = (model_part + extra - ld_block.astype(jnp.float32)).astype(jnp.bfloat16)
        return 4.0 * jnp.dot(misfit, factor_low, preferred_element_type=jnp.float32)

    result = lax.map(one_block, (jnp.arange(count, dtype=jnp.int32), ld_blocks))
    return result.reshape(M, K)
```

```python
import functools

import jax
import jax.numpy as jnp
from jax import lax
from jax.experimental import pallas as pl
from jax.experimental.pallas import tpu as pltpu
from jax.sharding import PartitionSpec as P

MESH = pl.DeviceIdType.MESH
F32, BF16 = jnp.float32, jnp.bfloat16
CHUNK = 256
LAG = 3
PIECES = 2
LANES = 128


def rows_at(start, count):
    return pl.ds(pl.multiple_of(start, count), count)


def flip(index, stride):
    return index + stride * (1 - 2 * (index // stride % 2))


def kernel(
    n_row, n_col, tiles, ld_ref, f32_ref, diag_ref, out_ref,
    tile, fac, panel, stage, keep, s1, r1, s2, r2, s3, r3, gsum, grecv, gfull,
    tile_sem, a_send, b_send, b_recv, c_send, line_recv, x_send, x_recv,
    s1_send, s1_recv, s2_send, s2_recv, s3_send, s3_recv, g_send, g_recv,
):
    r, c = lax.axis_index("row"), lax.axis_index("col")
    own, rank = fac.shape
    n_hi = n_col // 4
    chunk = s2.shape[1]
    nm = own // chunk
    steps = n_hi * nm
    far = (n_hi - 1) * nm
    core, mid, hi = c % 2, c // 2 % 2, c // 4
    half = rank // 2

    def remote(src, dst, send, recv, row, col):
        return pltpu.make_async_remote_copy(
            src_ref=src, dst_ref=dst, send_sem=send, recv_sem=recv,
            device_id=(row, col), device_id_type=MESH,
        )

    mirrored = hi >= n_hi // 2
    near = jnp.where(mirrored, n_hi - 1 - hi, hi)

    def target(t):
        ahead = n_hi - 1 - t
        behind = t - (n_hi - 1 - near)
        other = jnp.where(t < n_hi - 1 - near, ahead, behind)
        tgt = jnp.where(t == n_hi - 1, near, other)
        return jnp.where(mirrored, n_hi - 1 - tgt, tgt)

    def shard_of(v):
        t, side, which = v // 4 // nm, v // 2 % 2, v % 2
        return 4 * target(t) + 2 * ((mid + 1 + side) % 2) + (core + 1 + which) % 2

    def fetch(v):
        start = shard_of(v) * own + v // 4 % nm * chunk
        return pltpu.make_async_copy(
            ld_ref.at[rows_at(start, chunk)], tile.at[v % tiles], tile_sem.at[v % tiles]
        )

    @pl.loop(0, tiles)
    def _(v):
        fetch(v).start()

    fac[...] = f32_ref[...].astype(BF16)
    mine = r * n_col + c

    def panel_rows(slot, start, count):
        return panel.at[rows_at(slot * own + start, count)]

    if n_row == 2:
        part = own // 2 // PIECES
        x_col = c

        def b_copy(p):
            return remote(
                fac.at[pl.ds(own // 2 + p * part, part)], stage.at[p],
                b_send.at[p], b_recv.at[p], 1 - r, x_col,
            )

        slot = mine % n_row
        a_col = mine // n_row
        c_col = ((1 - r) * n_col + c) // n_row
        c_slot = ((1 - r) * n_col + c) % n_row

        def a_copy(p):
            return remote(
                fac.at[pl.ds(p * part, part)], panel_rows(slot, p * part, part),
                a_send.at[p], line_recv.at[slot, p], r, a_col,
            )

        def c_copy(p):
            return remote(
                stage.at[p], panel_rows(c_slot, own // 2 + p * part, part),
                c_send.at[p], line_recv.at[c_slot, p], r, c_col,
            )

        source_row = n_row * c // n_col
        line_half = jnp.where(source_row == r, 0, own // 2)

        def line_wait(j, p):
            remote(
                stage.at[0], panel_rows(j, line_half + p * part, part),
                c_send.at[0], line_recv.at[j, p], r, c,
            ).wait_recv()

        def x_copy(j, p):
            piece = panel_rows(j, line_half + p * part, part)
            return remote(piece, piece, x_send.at[j, p], x_recv.at[j, p], 1 - r, c)

        def x_wait(j, p):
            piece = panel_rows(j, own // 2 - line_half + p * part, part)
            remote(piece, piece, x_send.at[j, p], x_recv.at[j, p], 1 - r, c).wait_recv()

        for p in range(PIECES):
            b_copy(p).start()

        @pl.when(a_col != c)
        def _():
            for p in range(PIECES):
                a_copy(p).start()

        @pl.when(a_col == c)
        def _():
            panel_rows(slot, 0, own // 2)[...] = fac[: own // 2, :]
    else:
        to_col, to_slot = mine // n_row, mine % n_row

        def to_row(k):
            return remote(
                fac, panel_rows(to_slot, 0, own), a_send.at[k], x_recv.at[0, to_slot],
                (r + k) % n_row, to_col,
            )

        home = to_col == c

        @pl.when(home)
        def _():
            panel_rows(to_slot, 0, own)[...] = fac[...]

        @pl.when(jnp.logical_not(home))
        def _():
            to_row(0).start()

        for k in range(1, n_row):
            to_row(k).start()

    gram = lax.dot_general(
        fac[...], fac[...], (((0,), (0,)), ((), ())), preferred_element_type=F32
    )
    gfull[...] = gram
    col_strides = [2 ** b for b in range(1, n_col.bit_length() - 1)]
    row_strides = [2 ** b for b in range(n_row.bit_length() - 1)]
    links = [("col", s) for s in col_strides] + [("row", s) for s in row_strides]
    n_ex = len(links) + 2

    def gram_half(which):
        return gfull.at[rows_at(which * half, half)]

    def gram_copy(e):
        if e == 0:
            src, row, col = gram_half(1 - core), r, flip(c, 1)
        elif e == n_ex - 1:
            src, row, col = gsum.at[e - 1], r, flip(c, 1)
        else:
            axis, stride = links[e - 1]
            src = gsum.at[e - 1]
            row = flip(r, stride) if axis == "row" else r
            col = flip(c, stride) if axis == "col" else c
        return remote(src, grecv.at[e], g_send.at[e], g_recv.at[e], row, col)

    def gram_step(e):
        gram_copy(e - 1).wait_recv()
        before = gram_half(core)[...] if e == 1 else gsum[e - 2]
        gsum[e - 1] = before + grecv[e - 1]
        gram_copy(e).start()

    gram_copy(0).start()

    if n_row == 2:
        for p in range(PIECES):
            b_copy(p).wait_recv()

            @pl.when(c_col != c)
            def _():
                c_copy(p).start()

            @pl.when(c_col == c)
            def _():
                panel_rows(c_slot, own // 2 + p * part, part)[...] = stage[p]

        gram_step(1)
        for p in range(PIECES):
            for j in range(n_row):
                @pl.when((n_row * c + j) % n_col != c)
                def _():
                    line_wait(j, p)

                x_copy(j, p).start()
        for p in range(PIECES):
            for j in range(n_row):
                x_wait(j, p)
    else:
        gram_step(1)
        for j in range(n_row):
            @pl.when(n_row * c + j != mine)
            def _():
                remote(
                    fac, panel_rows(j, 0, own), a_send.at[0], x_recv.at[0, j], r, c
                ).wait_recv()

    def first(u):
        return remote(s1.at[u], r1.at[u], s1_send.at[u], s1_recv.at[u], r, flip(c, 1))

    def second(i):
        return remote(s2.at[i], r2.at[i], s2_send.at[i], s2_recv.at[i], r, flip(c, 2))

    def third(j, way, tgt, m):
        col = jnp.where(way == 0, c + 4, c - 4)
        return remote(
            s3.at[j], r3.at[way, tgt, m], s3_send.at[j], s3_recv.at[way, tgt, m], r, col
        )

    def compute(v):
        fetch(v).wait()
        acc = jnp.dot(tile[v % tiles], panel[...], preferred_element_type=F32)

        @pl.when(v + tiles < 4 * steps)
        def _():
            fetch(v + tiles).start()

        return acc

    def diagonal(v, ref):
        j = r * n_col + shard_of(v) - n_row * c

        @pl.when((j >= 0) & (j < n_row))
        def _():
            base = j * own + v // 4 % nm * chunk
            line = lax.broadcasted_iota(jnp.int32, (LANES, LANES), 0)
            lane = lax.broadcasted_iota(jnp.int32, (LANES, LANES), 1)
            for q in range(chunk // LANES):
                at = rows_at(base + q * LANES, LANES)
                values = jnp.broadcast_to(diag_ref[:, at].astype(F32), (LANES, LANES))
                square = jnp.where(line == lane, values, 0.0).astype(BF16)
                ref[pl.ds(q * LANES, LANES), :] -= jnp.dot(
                    square, panel[at, :], preferred_element_type=F32
                )

    def to_next(j):
        t, m = j // nm, j % nm
        tgt = target(t)
        way = jnp.where(tgt > hi, 0, 1)
        inner = jnp.where(way == 0, hi, n_hi - 1 - hi) > 0
        first(2 * j + 1).wait_recv()
        second(j).wait_recv()
        acc = keep[2 * j + 1] + r1[2 * j + 1].astype(F32) + r2[j].astype(F32)

        @pl.when(inner)
        def _():
            third(j, way, tgt, m).wait_recv()
            s3[j] = (acc + r3[way, tgt, m].astype(F32)).astype(BF16)

        @pl.when(jnp.logical_not(inner))
        def _():
            s3[j] = acc.astype(BF16)

        third(j, way, tgt, m).start()

    @pl.loop(0, steps)
    def _(i):
        for side in range(2):
            u = 2 * i + side
            scratch = keep.at[2 * steps]
            scratch[...] = compute(2 * u)
            diagonal(2 * u, scratch)
            s1[u] = scratch[...].astype(BF16)
            first(u).start()
            keep[u] = compute(2 * u + 1)
            diagonal(2 * u + 1, keep.at[u])
        first(2 * i).wait_recv()
        s2[i] = (keep[2 * i] + r1[2 * i].astype(F32)).astype(BF16)
        second(i).start()

        @pl.when((i >= LAG) & (i - LAG < far))
        def _():
            to_next(i - LAG)

        for e in range(2, n_ex):
            if e - 1 < steps:
                @pl.when(i == e - 1)
                def _():
                    gram_step(e)

    for e in range(max(2, steps + 1), n_ex):
        gram_step(e)

    if steps - LAG < far:
        @pl.loop(max(steps - LAG, 0), far)
        def _(j):
            to_next(j)

    gram_copy(n_ex - 1).wait_recv()
    gram_copy(0).wait_send()
    gram_half(core)[...] = gsum[n_ex - 2]
    gram_half(1 - core)[...] = grecv[n_ex - 1]
    total = gfull[...]
    total_hi = total.astype(BF16)
    total_lo = (total - total_hi.astype(F32)).astype(BF16)

    @pl.loop(0, nm)
    def _(m):
        rows = rows_at(m * chunk, chunk)
        model = jnp.dot(fac[rows, :], total_hi, preferred_element_type=F32)
        model += jnp.dot(fac[rows, :], total_lo, preferred_element_type=F32)
        out_ref[rows, :] = model

    @pl.loop(0, nm)
    def _(m):
        j = far + m
        rows = rows_at(m * chunk, chunk)
        first(2 * j + 1).wait_recv()
        out_ref[rows, :] -= keep[2 * j + 1] + r1[2 * j + 1].astype(F32)

        @pl.when(hi > 0)
        def _():
            third(0, 0, hi, m).wait_recv()
            out_ref[rows, :] -= r3[0, hi, m].astype(F32)

        @pl.when(hi < n_hi - 1)
        def _():
            third(0, 1, hi, m).wait_recv()
            out_ref[rows, :] -= r3[1, hi, m].astype(F32)

        second(j).wait_recv()
        out_ref[rows, :] = 4.0 * (out_ref[rows, :] - r2[j].astype(F32))

    if n_row == 2:
        for p in range(PIECES):
            b_copy(p).wait_send()

            @pl.when(a_col != c)
            def _():
                a_copy(p).wait_send()

            @pl.when(c_col != c)
            def _():
                c_copy(p).wait_send()

            for j in range(n_row):
                x_copy(j, p).wait_send()
    else:
        @pl.when(jnp.logical_not(home))
        def _():
            to_row(0).wait_send()

        for k in range(1, n_row):
            to_row(k).wait_send()
    for e in range(1, n_ex):
        gram_copy(e).wait_send()

    @pl.loop(0, steps)
    def _(i):
        first(2 * i).wait_send()
        first(2 * i + 1).wait_send()
        second(i).wait_send()

    @pl.loop(0, far)
    def _(j):
        tgt = target(j // nm)
        third(j, jnp.where(tgt > hi, 0, 1), tgt, j % nm).wait_send()


def local(ld_matrix, factor, diag_values):
    n_row, n_col = lax.axis_size("row"), lax.axis_size("col")
    own, rank = factor.shape
    width = ld_matrix.shape[1]
    n_hi = n_col // 4
    chunk = min(CHUNK, own)
    nm = own // chunk
    steps = n_hi * nm
    far = (n_hi - 1) * nm
    tiles = min(22, 4 * steps)
    n_ex = n_col.bit_length() - 2 + n_row.bit_length() - 1 + 2
    dma = lambda *shape: pltpu.SemaphoreType.DMA(shape)
    sums = lambda *n: pltpu.VMEM((*n, chunk, rank), BF16)
    gram = pltpu.VMEM((n_ex, rank // 2, rank), F32)
    vmem = pl.BlockSpec(memory_space=pltpu.VMEM)
    pieces = max(PIECES, n_row)
    return pl.pallas_call(
        functools.partial(kernel, n_row, n_col, tiles),
        out_shape=jax.ShapeDtypeStruct((own, rank), F32),
        in_specs=[pl.BlockSpec(memory_space=pl.ANY), vmem, vmem],
        out_specs=vmem,
        scratch_shapes=[
            pltpu.VMEM((tiles, chunk, width), BF16),
            pltpu.VMEM((own, rank), BF16),
            pltpu.VMEM((width, rank), BF16),
            pltpu.VMEM((PIECES, own // 2 // PIECES, rank), BF16),
            pltpu.VMEM((2 * steps + 1, chunk, rank), F32),
            sums(2 * steps), sums(2 * steps), sums(steps), sums(steps),
            sums(far), sums(2, n_hi, nm),
            gram, gram, pltpu.VMEM((rank, rank), F32),
            dma(tiles), dma(pieces), dma(PIECES), dma(PIECES), dma(PIECES),
            dma(n_row, PIECES), dma(n_row, pieces), dma(n_row, pieces),
            dma(2 * steps), dma(2 * steps), dma(steps), dma(steps),
            dma(far), dma(2, n_hi, nm), dma(n_ex), dma(n_ex),
        ],
        compiler_params=pltpu.CompilerParams(
            has_side_effects=True, vmem_limit_bytes=62 * 2**20
        ),
    )(ld_matrix, factor, diag_values[None, :])


def solution(mesh):
    in_specs = (P("row", "col"), P(("row", "col"), None), P("col"))
    out_specs = P(("row", "col"), None)
    return jax.shard_map(local, mesh=mesh, in_specs=in_specs, out_specs=out_specs, check_vma=False)
```

```python
import functools

import jax
import jax.numpy as jnp
from jax import lax
from jax.experimental import pallas as pl
from jax.experimental.pallas import tpu as pltpu
from jax.sharding import PartitionSpec as P

MESH = pl.DeviceIdType.MESH
F32, BF16 = jnp.float32, jnp.bfloat16
CHUNK = 256
LAG = 3
PACE = 3
SLOTS = 6
PARTS = 16
ALONE = 4
LANES = 128


def rows_at(start, count):
    return pl.ds(pl.multiple_of(start, count), count)


def flip(index, stride):
    return index + stride * (1 - 2 * (index // stride % 2))


def kernel(
    n_row, n_col, slots, ld_ref, f32_ref, diag_ref, out_ref,
    tile, wide, fac, diag, panel, stage, acc, keep, result,
    s1, r1, s2, r2, s3, r3, gsum, grecv, gfull,
    tile_sem, in_sem, out_sem, a_send, b_send, b_recv, c_send, line_recv, x_send, x_recv,
    s1_send, s1_recv, s2_send, s2_recv, s3_send, s3_recv, g_send, g_recv,
):
    r, c = lax.axis_index("row"), lax.axis_index("col")
    own, rank = fac.shape
    n_hi = n_col // 4
    chunk = s2.shape[1]
    nm = own // chunk
    steps = n_hi * nm
    far = (n_hi - 1) * nm
    core, mid, hi = c % 2, c // 2 % 2, c // 4
    half = rank // 2
    part = own // PARTS
    mine = r * n_col + c
    col_strides = [2 ** b for b in range(1, n_col.bit_length() - 1)]
    row_strides = [2 ** b for b in range(n_row.bit_length() - 1)]

    def remote(src, dst, send, recv, row, col):
        return pltpu.make_async_remote_copy(
            src_ref=src, dst_ref=dst, send_sem=send, recv_sem=recv,
            device_id=(row, col), device_id_type=MESH,
        )

    a_col, a_slot = mine // n_row, mine % n_row
    twin = (1 - r) * n_col + c
    c_col, c_slot = twin // n_row, twin % n_row

    if n_row == 2:
        barrier = pltpu.get_barrier_semaphore()
        greeted = [(r, flip(c, s)) for s in [1] + col_strides] + [(1 - r, c)]
        greeted += [(r, col) for col in (a_col, c_col, 2 * c % n_col, (2 * c + 1) % n_col)]
        greeted += [(r, jnp.where(hi < n_hi - 1, c + 4, c)), (r, jnp.where(hi > 0, c - 4, c))]
        others = [jnp.where((row != r) | (col != c), 1, 0) for row, col in greeted]
        for (row, col), other in zip(greeted, others):
            @pl.when(other == 1)
            def _():
                pl.semaphore_signal(barrier, inc=1, device_id=(row, col), device_id_type=MESH)

    load = pltpu.make_async_copy(f32_ref, wide, in_sem)
    load.start()

    mirrored = hi >= n_hi // 2
    near = jnp.where(mirrored, n_hi - 1 - hi, hi)

    def target(t):
        ahead = n_hi - 1 - t
        behind = t - (n_hi - 1 - near)
        other = jnp.where(t < n_hi - 1 - near, ahead, behind)
        tgt = jnp.where(t == n_hi - 1, near, other)
        return jnp.where(mirrored, n_hi - 1 - tgt, tgt)

    def shard_of(i, side, which):
        return 4 * target(i // nm) + 2 * ((mid + 1 + side) % 2) + (core + 1 + which) % 2

    def fetch(i, side, which):
        start = shard_of(i, side, which) * own + i % nm * chunk
        return pltpu.make_async_copy(
            ld_ref.at[rows_at(start, chunk)],
            tile.at[i % slots, side, pl.ds(which * chunk, chunk)],
            tile_sem.at[i % slots, side, which],
        )

    @pl.loop(0, slots)
    def _(i):
        for side in range(2):
            for which in range(2):
                fetch(i, side, which).start()

    diag[...] = diag_ref[...].astype(F32)
    load.wait()
    fac[...] = wide[...].astype(BF16)

    links = [("col", 1), ("col", 2), ("row", 1)]
    links += [("col", s) for s in col_strides[1:]] + [("row", s) for s in row_strides[1:]]
    links += [("row", 1), ("col", 1)]
    n_ex = len(links)
    quarter = half // 2
    r_low = r % 2

    def gram_half(which):
        return gfull.at[rows_at(which * half, half)]

    def gram_copy(e):
        axis, stride = links[e]
        row = flip(r, stride) if axis == "row" else r
        col = flip(c, stride) if axis == "col" else c
        if e == 0:
            src, dst = gram_half(1 - core), grecv.at[0]
        elif e in (1, n_ex - 1):
            src, dst = gsum.at[e - 1], grecv.at[e]
        elif e == 2:
            src, dst = gsum.at[1, rows_at((1 - r_low) * quarter, quarter)], grecv.at[2, :quarter]
        else:
            src, dst = gsum.at[e - 1, :quarter], grecv.at[e, :quarter]
        return remote(src, dst, g_send.at[e], g_recv.at[e], row, col)

    def gram_start():
        gfull[...] = lax.dot_general(
            fac[...], fac[...], (((0,), (0,)), ((), ())), preferred_element_type=F32
        )
        gram_copy(0).start()

    def gram_step(e):
        gram_copy(e - 1).wait_recv()
        if e == 1:
            gsum[0] = gram_half(core)[...] + grecv[0]
        elif e == 2:
            gsum[1] = gsum[0] + grecv[1]
        elif e == 3:
            gsum[2, :quarter] = gsum[1, rows_at(r_low * quarter, quarter)] + grecv[2, :quarter]
        elif e < n_ex - 1:
            gsum[e - 1, :quarter] = gsum[e - 2, :quarter] + grecv[e - 1, :quarter]
        else:
            gsum[e - 1, rows_at(r_low * quarter, quarter)] = gsum[e - 2, :quarter]
            gsum[e - 1, rows_at((1 - r_low) * quarter, quarter)] = grecv[e - 1, :quarter]
        gram_copy(e).start()

    def panel_rows(slot, start, count):
        return panel.at[pl.ds(pl.multiple_of(slot * own + start, part), count)]

    if n_row == 2:
        on_both = range(2 * ALONE, PARTS)
        on_own = [*range(ALONE), *on_both]
        on_twin = [*range(ALONE, 2 * ALONE), *on_both]

        def a_copy(q):
            return remote(
                fac.at[pl.ds(q * part, part)], panel_rows(a_slot, q * part, part),
                a_send.at[q], line_recv.at[a_slot, q], r, a_col,
            )

        def b_copy(q):
            return remote(
                fac.at[pl.ds(q * part, part)], stage.at[q], b_send.at[q], b_recv.at[q], 1 - r, c
            )

        def c_copy(q):
            return remote(
                stage.at[q], panel_rows(c_slot, q * part, part),
                c_send.at[q], line_recv.at[c_slot, q], r, c_col,
            )

        from_own = n_row * c // n_col == r
        near_at = jnp.where(from_own, 0, ALONE)

        def line_wait(j, q):
            remote(
                stage.at[0], panel_rows(j, q * part, part),
                c_send.at[0], line_recv.at[j, q], r, c,
            ).wait_recv()

        def x_copy(j, p, at):
            piece = panel_rows(j, (at + p) * part, part)
            return remote(piece, piece, x_send.at[j, p], x_recv.at[j, p], 1 - r, c)

        pl.semaphore_wait(barrier, sum(others))
        for q in on_twin:
            b_copy(q).start()

        @pl.when(a_col != c)
        def _():
            for q in on_own:
                a_copy(q).start()

        @pl.when(a_col == c)
        def _():
            for q in on_own:
                panel_rows(a_slot, q * part, part)[...] = fac[q * part : (q + 1) * part, :]

        gram_start()
        for n, q in enumerate(on_twin):
            b_copy(q).wait_recv()

            @pl.when(c_col != c)
            def _():
                c_copy(q).start()

            @pl.when(c_col == c)
            def _():
                panel_rows(c_slot, q * part, part)[...] = stage[q]

            if n == 1:
                gram_step(1)
        for p in range(ALONE):
            for j in range(n_row):
                @pl.when((n_row * c + j) % n_col != c)
                def _():
                    line_wait(j, near_at + p)

                x_copy(j, p, near_at).start()
        for q in on_both:
            for j in range(n_row):
                @pl.when((n_row * c + j) % n_col != c)
                def _():
                    line_wait(j, q)
        for p in range(ALONE):
            for j in range(n_row):
                x_copy(j, p, ALONE - near_at).wait_recv()
    else:
        def to_row(k):
            return remote(
                fac, panel_rows(a_slot, 0, own), a_send.at[k], x_recv.at[a_slot, 0],
                (r + k) % n_row, a_col,
            )

        @pl.when(a_col == c)
        def _():
            panel_rows(a_slot, 0, own)[...] = fac[...]

        @pl.when(a_col != c)
        def _():
            to_row(0).start()

        for k in range(1, n_row):
            to_row(k).start()
        gram_start()
        gram_step(1)
        for j in range(n_row):
            @pl.when(n_row * c + j != mine)
            def _():
                remote(
                    fac, panel_rows(j, 0, own), a_send.at[0], x_recv.at[j, 0], r, c
                ).wait_recv()

    def first(u):
        return remote(s1.at[u], r1.at[u], s1_send.at[u], s1_recv.at[u], r, flip(c, 1))

    def second(i):
        return remote(s2.at[i], r2.at[i], s2_send.at[i], s2_recv.at[i], r, flip(c, 2))

    def third(j, way, tgt, m):
        col = jnp.where(way == 0, c + 4, c - 4)
        return remote(
            s3.at[j], r3.at[way, tgt, m], s3_send.at[j], s3_recv.at[way, tgt, m], r, col
        )

    def diagonal(i, side, which):
        j = r * n_col + shard_of(i, side, which) - n_row * c

        @pl.when((j >= 0) & (j < n_row))
        def _():
            base = (j * own + i % nm * chunk) // LANES
            line = lax.broadcasted_iota(jnp.int32, (LANES, LANES), 0)
            lane = lax.broadcasted_iota(jnp.int32, (LANES, LANES), 1)
            for q in range(chunk // LANES):
                values = jnp.broadcast_to(diag[pl.ds(base + q, 1), :], (LANES, LANES))
                square = jnp.where(line == lane, values, 0.0).astype(BF16)
                acc[side, pl.ds(which * chunk + q * LANES, LANES), :] -= jnp.dot(
                    square, panel[rows_at((base + q) * LANES, LANES), :],
                    preferred_element_type=F32,
                )

    def pace(e):
        return 1 + PACE * (e - 2)

    def to_next(j):
        t, m = j // nm, j % nm
        tgt = target(t)
        way = jnp.where(tgt > hi, 0, 1)
        inner = jnp.where(way == 0, hi, n_hi - 1 - hi) > 0
        first(2 * j + 1).wait_recv()
        second(j).wait_recv()
        part_sum = keep[j] + r1[2 * j + 1].astype(F32) + r2[j].astype(F32)

        @pl.when(inner)
        def _():
            third(j, way, tgt, m).wait_recv()
            s3[j] = (part_sum + r3[way, tgt, m].astype(F32)).astype(BF16)

        @pl.when(jnp.logical_not(inner))
        def _():
            s3[j] = part_sum.astype(BF16)

        third(j, way, tgt, m).start()

    @pl.loop(0, steps)
    def _(i):
        for side in range(2):
            for which in range(2):
                fetch(i, side, which).wait()
            acc[side] = jnp.dot(tile[i % slots, side], panel[...], preferred_element_type=F32)

            @pl.when(i + slots < steps)
            def _():
                for which in range(2):
                    fetch(i + slots, side, which).start()

            for which in range(2):
                diagonal(i, side, which)
            s1[2 * i + side] = acc[side, :chunk, :].astype(BF16)
            first(2 * i + side).start()
        keep[i] = acc[1, chunk:, :]
        first(2 * i).wait_recv()
        s2[i] = (acc[0, chunk:, :] + r1[2 * i].astype(F32)).astype(BF16)
        second(i).start()

        @pl.when((i >= LAG) & (i - LAG < far))
        def _():
            to_next(i - LAG)

        for e in range(2, n_ex):
            if pace(e) < steps:
                @pl.when(i == pace(e))
                def _():
                    gram_step(e)

    for e in range(2, n_ex):
        if pace(e) >= steps:
            gram_step(e)

    if steps - LAG < far:
        @pl.loop(max(steps - LAG, 0), far)
        def _(j):
            to_next(j)

    gram_copy(n_ex - 1).wait_recv()
    gram_copy(0).wait_send()
    gram_half(core)[...] = gsum[n_ex - 2]
    gram_half(1 - core)[...] = grecv[n_ex - 1]
    total = gfull[...]
    total_hi = total.astype(BF16)
    total_lo = (total - total_hi.astype(F32)).astype(BF16)

    @pl.loop(0, nm)
    def _(m):
        rows = rows_at(m * chunk, chunk)
        model = jnp.dot(fac[rows, :], total_hi, preferred_element_type=F32)
        model += jnp.dot(fac[rows, :], total_lo, preferred_element_type=F32)
        result[rows, :] = model

    def put(m):
        rows = rows_at(m * chunk, chunk)
        return pltpu.make_async_copy(result.at[rows], out_ref.at[rows], out_sem.at[m])

    @pl.loop(0, nm)
    def _(m):
        j = far + m
        rows = rows_at(m * chunk, chunk)
        first(2 * j + 1).wait_recv()
        result[rows, :] -= keep[j] + r1[2 * j + 1].astype(F32)

        @pl.when(hi > 0)
        def _():
            third(0, 0, hi, m).wait_recv()
            result[rows, :] -= r3[0, hi, m].astype(F32)

        @pl.when(hi < n_hi - 1)
        def _():
            third(0, 1, hi, m).wait_recv()
            result[rows, :] -= r3[1, hi, m].astype(F32)

        second(j).wait_recv()
        result[rows, :] = 4.0 * (result[rows, :] - r2[j].astype(F32))
        put(m).start()

    if n_row == 2:
        for q in on_twin:
            b_copy(q).wait_send()

        @pl.when(a_col != c)
        def _():
            for q in on_own:
                a_copy(q).wait_send()

        @pl.when(c_col != c)
        def _():
            for q in on_twin:
                c_copy(q).wait_send()

        for p in range(ALONE):
            for j in range(n_row):
                x_copy(j, p, near_at).wait_send()
    else:
        @pl.when(a_col != c)
        def _():
            to_row(0).wait_send()

        for k in range(1, n_row):
            to_row(k).wait_send()
    for e in range(1, n_ex):
        gram_copy(e).wait_send()

    @pl.loop(0, steps)
    def _(i):
        first(2 * i).wait_send()
        first(2 * i + 1).wait_send()
        second(i).wait_send()

    @pl.loop(0, far)
    def _(j):
        tgt = target(j // nm)
        third(j, jnp.where(tgt > hi, 0, 1), tgt, j % nm).wait_send()

    @pl.loop(0, nm)
    def _(m):
        put(m).wait()


def local(ld_matrix, factor, diag_values):
    n_row, n_col = lax.axis_size("row"), lax.axis_size("col")
    own, rank = factor.shape
    width = ld_matrix.shape[1]
    n_hi = n_col // 4
    chunk = min(CHUNK, own)
    nm = own // chunk
    steps = n_hi * nm
    far = (n_hi - 1) * nm
    slots = min(SLOTS, steps)
    n_ex = n_col.bit_length() - 1 + n_row.bit_length() - 1 + 2
    dma = lambda *shape: pltpu.SemaphoreType.DMA(shape)
    sums = lambda *n: pltpu.VMEM((*n, chunk, rank), BF16)
    gram = pltpu.VMEM((n_ex, rank // 2, rank), F32)
    anywhere = pl.BlockSpec(memory_space=pl.ANY)
    own_barrier = dict(collective_id=0) if n_row == 2 else {}
    return pl.pallas_call(
        functools.partial(kernel, n_row, n_col, slots),
        out_shape=jax.ShapeDtypeStruct((own, rank), F32),
        in_specs=[anywhere, anywhere, pl.BlockSpec(memory_space=pltpu.VMEM)],
        out_specs=anywhere,
        scratch_shapes=[
            pltpu.VMEM((slots, 2, 2 * chunk, width), BF16),
            pltpu.VMEM((own, rank), F32),
            pltpu.VMEM((own, rank), BF16),
            pltpu.VMEM((width // LANES, LANES), F32),
            pltpu.VMEM((width, rank), BF16),
            pltpu.VMEM((PARTS, own // PARTS, rank), BF16),
            pltpu.VMEM((2, 2 * chunk, rank), F32),
            pltpu.VMEM((steps, chunk, rank), F32),
            pltpu.VMEM((own, rank), F32),
            sums(2 * steps), sums(2 * steps), sums(steps), sums(steps),
            sums(far), sums(2, n_hi, nm),
            gram, gram, pltpu.VMEM((rank, rank), F32),
            dma(slots, 2, 2), pltpu.SemaphoreType.DMA, dma(nm),
            dma(PARTS), dma(PARTS), dma(PARTS), dma(PARTS),
            dma(n_row, PARTS), dma(n_row, PARTS), dma(n_row, PARTS),
            dma(2 * steps), dma(2 * steps), dma(steps), dma(steps),
            dma(far), dma(2, n_hi, nm), dma(n_ex), dma(n_ex),
        ],
        compiler_params=pltpu.CompilerParams(
            has_side_effects=True, vmem_limit_bytes=63 * 2**20, **own_barrier
        ),
    )(ld_matrix, factor, diag_values.reshape(width // LANES, LANES))


def solution(mesh):
    in_specs = (P("row", "col"), P(("row", "col"), None), P("col"))
    out_specs = P(("row", "col"), None)
    return jax.shard_map(local, mesh=mesh, in_specs=in_specs, out_specs=out_specs, check_vma=False)
```

```python
import functools

import jax
import jax.numpy as jnp
from jax import lax
from jax.experimental import pallas as pl
from jax.experimental.pallas import tpu as pltpu
from jax.sharding import PartitionSpec as P

MESH = pl.DeviceIdType.MESH
F32, BF16 = jnp.float32, jnp.bfloat16
CHUNK = 256
LAG = 3
PACE = 4
SLOTS = 6
PARTS = 16
OWN, TWIN = 4, 4
LANES = 128


def rows_at(start, count):
    return pl.ds(pl.multiple_of(start, count), count)


def flip(index, stride):
    return index + stride * (1 - 2 * (index // stride % 2))


def kernel(
    n_row, n_col, slots, ld_ref, f32_ref, diag_ref, out_ref,
    tile, wide, fac, diag, panel, stage, acc, keep, result,
    s1, r1, s2, r2, s3, r3, gsum, grecv, gfull,
    tile_sem, in_sem, out_sem, a_send, b_send, b_recv, c_send, line_recv, x_send, x_recv,
    s1_send, s1_recv, s2_send, s2_recv, s3_send, s3_recv, g_send, g_recv,
):
    r, c = lax.axis_index("row"), lax.axis_index("col")
    own, rank = fac.shape
    n_hi = n_col // 4
    chunk = s2.shape[1]
    nm = own // chunk
    steps = n_hi * nm
    far = (n_hi - 1) * nm
    core, mid, hi = c % 2, c // 2 % 2, c // 4
    half = rank // 2
    part = own // PARTS
    mine = r * n_col + c
    col_strides = [2 ** b for b in range(1, n_col.bit_length() - 1)]
    row_strides = [2 ** b for b in range(n_row.bit_length() - 1)]

    def remote(src, dst, send, recv, row, col):
        return pltpu.make_async_remote_copy(
            src_ref=src, dst_ref=dst, send_sem=send, recv_sem=recv,
            device_id=(row, col), device_id_type=MESH,
        )

    a_col, a_slot = mine // n_row, mine % n_row
    twin = (1 - r) * n_col + c
    c_col, c_slot = twin // n_row, twin % n_row

    if n_row == 2:
        barrier = pltpu.get_barrier_semaphore()
        greeted = [(r, flip(c, s)) for s in [1] + col_strides] + [(1 - r, c)]
        greeted += [(r, col) for col in (a_col, c_col, 2 * c % n_col, (2 * c + 1) % n_col)]
        greeted += [(r, jnp.where(hi < n_hi - 1, c + 4, c)), (r, jnp.where(hi > 0, c - 4, c))]
        others = [jnp.where((row != r) | (col != c), 1, 0) for row, col in greeted]
        for (row, col), other in zip(greeted, others):
            @pl.when(other == 1)
            def _():
                pl.semaphore_signal(barrier, inc=1, device_id=(row, col), device_id_type=MESH)

    load = pltpu.make_async_copy(f32_ref, wide, in_sem)
    load.start()

    mirrored = hi >= n_hi // 2
    near = jnp.where(mirrored, n_hi - 1 - hi, hi)

    def target(t):
        ahead = n_hi - 1 - t
        behind = t - (n_hi - 1 - near)
        other = jnp.where(t < n_hi - 1 - near, ahead, behind)
        tgt = jnp.where(t == n_hi - 1, near, other)
        return jnp.where(mirrored, n_hi - 1 - tgt, tgt)

    def shard_of(i, side, which):
        return 4 * target(i // nm) + 2 * ((mid + 1 + side) % 2) + (core + 1 + which) % 2

    def fetch(i, side, which):
        start = shard_of(i, side, which) * own + i % nm * chunk
        return pltpu.make_async_copy(
            ld_ref.at[rows_at(start, chunk)],
            tile.at[i % slots, side, pl.ds(which * chunk, chunk)],
            tile_sem.at[i % slots, side, which],
        )

    @pl.loop(0, slots)
    def _(i):
        for side in range(2):
            for which in range(2):
                fetch(i, side, which).start()

    diag[...] = diag_ref[...].astype(F32)
    load.wait()
    fac[...] = wide[...].astype(BF16)

    links = [("col", 1), ("col", 2), ("row", 1)]
    links += [("col", s) for s in col_strides[1:]] + [("row", s) for s in row_strides[1:]]
    links += [("row", 1), ("col", 1)]
    n_ex = len(links)
    quarter = half // 2
    r_low = r % 2

    def gram_half(which):
        return gfull.at[rows_at(which * half, half)]

    def gram_copy(e):
        axis, stride = links[e]
        row = flip(r, stride) if axis == "row" else r
        col = flip(c, stride) if axis == "col" else c
        if e == 0:
            src, dst = gram_half(1 - core), grecv.at[0]
        elif e in (1, n_ex - 1):
            src, dst = gsum.at[e - 1], grecv.at[e]
        elif e == 2:
            src, dst = gsum.at[1, rows_at((1 - r_low) * quarter, quarter)], grecv.at[2, :quarter]
        else:
            src, dst = gsum.at[e - 1, :quarter], grecv.at[e, :quarter]
        return remote(src, dst, g_send.at[e], g_recv.at[e], row, col)

    def gram_start():
        gfull[...] = lax.dot_general(
            fac[...], fac[...], (((0,), (0,)), ((), ())), preferred_element_type=F32
        )
        gram_copy(0).start()

    def gram_step(e):
        gram_copy(e - 1).wait_recv()
        if e == 1:
            gsum[0] = gram_half(core)[...] + grecv[0]
        elif e == 2:
            gsum[1] = gsum[0] + grecv[1]
        elif e == 3:
            gsum[2, :quarter] = gsum[1, rows_at(r_low * quarter, quarter)] + grecv[2, :quarter]
        elif e < n_ex - 1:
            gsum[e - 1, :quarter] = gsum[e - 2, :quarter] + grecv[e - 1, :quarter]
        else:
            gsum[e - 1, rows_at(r_low * quarter, quarter)] = gsum[e - 2, :quarter]
            gsum[e - 1, rows_at((1 - r_low) * quarter, quarter)] = grecv[e - 1, :quarter]
        gram_copy(e).start()

    def panel_rows(slot, start, count):
        return panel.at[pl.ds(pl.multiple_of(slot * own + start, part), count)]

    if n_row == 2:
        own_only, twin_only = range(OWN), range(OWN, OWN + TWIN)
        on_both = range(OWN + TWIN, PARTS)
        on_own, on_twin = [*own_only, *on_both], [*twin_only, *on_both]

        def a_copy(q):
            return remote(
                fac.at[pl.ds(q * part, part)], panel_rows(a_slot, q * part, part),
                a_send.at[q], line_recv.at[a_slot, q], r, a_col,
            )

        def b_copy(q):
            return remote(
                fac.at[pl.ds(q * part, part)], stage.at[q], b_send.at[q], b_recv.at[q], 1 - r, c
            )

        def c_copy(q):
            return remote(
                stage.at[q], panel_rows(c_slot, q * part, part),
                c_send.at[q], line_recv.at[c_slot, q], r, c_col,
            )

        from_own = n_row * c // n_col == r

        def line_wait(j, q):
            remote(
                stage.at[0], panel_rows(j, q * part, part),
                c_send.at[0], line_recv.at[j, q], r, c,
            ).wait_recv()

        def x_copy(j, q):
            piece = panel_rows(j, q * part, part)
            return remote(piece, piece, x_send.at[j, q], x_recv.at[j, q], 1 - r, c)

        def from_line(j, q):
            @pl.when((n_row * c + j) % n_col != c)
            def _():
                line_wait(j, q)

        def meet(here, there):
            for q in here:
                for j in range(n_row):
                    from_line(j, q)
                    x_copy(j, q).start()
            for q in on_both:
                for j in range(n_row):
                    from_line(j, q)
            for q in there:
                for j in range(n_row):
                    x_copy(j, q).wait_recv()

        pl.semaphore_wait(barrier, sum(others))
        for q in on_twin:
            b_copy(q).start()

        @pl.when(a_col != c)
        def _():
            for q in on_own:
                a_copy(q).start()

        @pl.when(a_col == c)
        def _():
            for q in on_own:
                panel_rows(a_slot, q * part, part)[...] = fac[q * part : (q + 1) * part, :]

        gram_start()
        for n, q in enumerate(on_twin):
            b_copy(q).wait_recv()

            @pl.when(c_col != c)
            def _():
                c_copy(q).start()

            @pl.when(c_col == c)
            def _():
                panel_rows(c_slot, q * part, part)[...] = stage[q]

            if n == 1:
                gram_step(1)

        @pl.when(from_own)
        def _():
            meet(own_only, twin_only)

        @pl.when(jnp.logical_not(from_own))
        def _():
            meet(twin_only, own_only)
    else:
        def to_row(k):
            return remote(
                fac, panel_rows(a_slot, 0, own), a_send.at[k], x_recv.at[a_slot, 0],
                (r + k) % n_row, a_col,
            )

        @pl.when(a_col == c)
        def _():
            panel_rows(a_slot, 0, own)[...] = fac[...]

        @pl.when(a_col != c)
        def _():
            to_row(0).start()

        for k in range(1, n_row):
            to_row(k).start()
        gram_start()
        gram_step(1)
        for j in range(n_row):
            @pl.when(n_row * c + j != mine)
            def _():
                remote(
                    fac, panel_rows(j, 0, own), a_send.at[0], x_recv.at[j, 0], r, c
                ).wait_recv()

    def first(u):
        return remote(s1.at[u], r1.at[u], s1_send.at[u], s1_recv.at[u], r, flip(c, 1))

    def second(i):
        return remote(s2.at[i], r2.at[i], s2_send.at[i], s2_recv.at[i], r, flip(c, 2))

    def third(j, way, tgt, m):
        col = jnp.where(way == 0, c + 4, c - 4)
        return remote(
            s3.at[j], r3.at[way, tgt, m], s3_send.at[j], s3_recv.at[way, tgt, m], r, col
        )

    def diagonal(i, side, which):
        j = r * n_col + shard_of(i, side, which) - n_row * c

        @pl.when((j >= 0) & (j < n_row))
        def _():
            base = (j * own + i % nm * chunk) // LANES
            line = lax.broadcasted_iota(jnp.int32, (LANES, LANES), 0)
            lane = lax.broadcasted_iota(jnp.int32, (LANES, LANES), 1)
            for q in range(chunk // LANES):
                values = jnp.broadcast_to(diag[pl.ds(base + q, 1), :], (LANES, LANES))
                square = jnp.where(line == lane, values, 0.0).astype(BF16)
                acc[side, pl.ds(which * chunk + q * LANES, LANES), :] -= jnp.dot(
                    square, panel[rows_at((base + q) * LANES, LANES), :],
                    preferred_element_type=F32,
                )

    def pace(e):
        return 1 + PACE * (e - 2)

    def to_next(j):
        t, m = j // nm, j % nm
        tgt = target(t)
        way = jnp.where(tgt > hi, 0, 1)
        inner = jnp.where(way == 0, hi, n_hi - 1 - hi) > 0
        first(2 * j + 1).wait_recv()
        second(j).wait_recv()
        part_sum = keep[j] + r1[2 * j + 1].astype(F32) + r2[j].astype(F32)

        @pl.when(inner)
        def _():
            third(j, way, tgt, m).wait_recv()
            s3[j] = (part_sum + r3[way, tgt, m].astype(F32)).astype(BF16)

        @pl.when(jnp.logical_not(inner))
        def _():
            s3[j] = part_sum.astype(BF16)

        third(j, way, tgt, m).start()

    @pl.loop(0, steps)
    def _(i):
        for side in range(2):
            for which in range(2):
                fetch(i, side, which).wait()
            acc[side] = jnp.dot(tile[i % slots, side], panel[...], preferred_element_type=F32)

            @pl.when(i + slots < steps)
            def _():
                for which in range(2):
                    fetch(i + slots, side, which).start()

            for which in range(2):
                diagonal(i, side, which)
            s1[2 * i + side] = acc[side, :chunk, :].astype(BF16)
            first(2 * i + side).start()
        keep[i] = acc[1, chunk:, :]
        first(2 * i).wait_recv()
        s2[i] = (acc[0, chunk:, :] + r1[2 * i].astype(F32)).astype(BF16)
        second(i).start()

        @pl.when((i >= LAG) & (i - LAG < far))
        def _():
            to_next(i - LAG)

        for e in range(2, n_ex):
            if pace(e) < steps:
                @pl.when(i == pace(e))
                def _():
                    gram_step(e)

    for e in range(2, n_ex):
        if pace(e) >= steps:
            gram_step(e)

    if steps - LAG < far:
        @pl.loop(max(steps - LAG, 0), far)
        def _(j):
            to_next(j)

    gram_copy(n_ex - 1).wait_recv()
    gram_copy(0).wait_send()
    gram_half(core)[...] = gsum[n_ex - 2]
    gram_half(1 - core)[...] = grecv[n_ex - 1]
    total = gfull[...]
    total_hi = total.astype(BF16)
    total_lo = (total - total_hi.astype(F32)).astype(BF16)

    @pl.loop(0, nm)
    def _(m):
        rows = rows_at(m * chunk, chunk)
        model = jnp.dot(fac[rows, :], total_hi, preferred_element_type=F32)
        model += jnp.dot(fac[rows, :], total_lo, preferred_element_type=F32)
        result[rows, :] = model

    def put(m):
        rows = rows_at(m * chunk, chunk)
        return pltpu.make_async_copy(result.at[rows], out_ref.at[rows], out_sem.at[m])

    @pl.loop(0, nm)
    def _(m):
        j = far + m
        rows = rows_at(m * chunk, chunk)
        first(2 * j + 1).wait_recv()
        result[rows, :] -= keep[j] + r1[2 * j + 1].astype(F32)

        @pl.when(hi > 0)
        def _():
            third(0, 0, hi, m).wait_recv()
            result[rows, :] -= r3[0, hi, m].astype(F32)

        @pl.when(hi < n_hi - 1)
        def _():
            third(0, 1, hi, m).wait_recv()
            result[rows, :] -= r3[1, hi, m].astype(F32)

        second(j).wait_recv()
        result[rows, :] = 4.0 * (result[rows, :] - r2[j].astype(F32))
        put(m).start()

    if n_row == 2:
        for q in on_twin:
            b_copy(q).wait_send()

        @pl.when(a_col != c)
        def _():
            for q in on_own:
                a_copy(q).wait_send()

        @pl.when(c_col != c)
        def _():
            for q in on_twin:
                c_copy(q).wait_send()

        for here, gone in ((from_own, own_only), (jnp.logical_not(from_own), twin_only)):
            @pl.when(here)
            def _():
                for q in gone:
                    for j in range(n_row):
                        x_copy(j, q).wait_send()
    else:
        @pl.when(a_col != c)
        def _():
            to_row(0).wait_send()

        for k in range(1, n_row):
            to_row(k).wait_send()
    for e in range(1, n_ex):
        gram_copy(e).wait_send()

    @pl.loop(0, steps)
    def _(i):
        first(2 * i).wait_send()
        first(2 * i + 1).wait_send()
        second(i).wait_send()

    @pl.loop(0, far)
    def _(j):
        tgt = target(j // nm)
        third(j, jnp.where(tgt > hi, 0, 1), tgt, j % nm).wait_send()

    @pl.loop(0, nm)
    def _(m):
        put(m).wait()


def local(ld_matrix, factor, diag_values):
    n_row, n_col = lax.axis_size("row"), lax.axis_size("col")
    own, rank = factor.shape
    width = ld_matrix.shape[1]
    n_hi = n_col // 4
    chunk = min(CHUNK, own)
    nm = own // chunk
    steps = n_hi * nm
    far = (n_hi - 1) * nm
    slots = min(SLOTS, steps)
    n_ex = n_col.bit_length() - 1 + n_row.bit_length() - 1 + 2
    dma = lambda *shape: pltpu.SemaphoreType.DMA(shape)
    sums = lambda *n: pltpu.VMEM((*n, chunk, rank), BF16)
    gram = pltpu.VMEM((n_ex, rank // 2, rank), F32)
    anywhere = pl.BlockSpec(memory_space=pl.ANY)
    own_barrier = dict(collective_id=0) if n_row == 2 else {}
    return pl.pallas_call(
        functools.partial(kernel, n_row, n_col, slots),
        out_shape=jax.ShapeDtypeStruct((own, rank), F32),
        in_specs=[anywhere, anywhere, pl.BlockSpec(memory_space=pltpu.VMEM)],
        out_specs=anywhere,
        scratch_shapes=[
            pltpu.VMEM((slots, 2, 2 * chunk, width), BF16),
            pltpu.VMEM((own, rank), F32),
            pltpu.VMEM((own, rank), BF16),
            pltpu.VMEM((width // LANES, LANES), F32),
            pltpu.VMEM((width, rank), BF16),
            pltpu.VMEM((PARTS, own // PARTS, rank), BF16),
            pltpu.VMEM((2, 2 * chunk, rank), F32),
            pltpu.VMEM((steps, chunk, rank), F32),
            pltpu.VMEM((own, rank), F32),
            sums(2 * steps), sums(2 * steps), sums(steps), sums(steps),
            sums(far), sums(2, n_hi, nm),
            gram, gram, pltpu.VMEM((rank, rank), F32),
            dma(slots, 2, 2), pltpu.SemaphoreType.DMA, dma(nm),
            dma(PARTS), dma(PARTS), dma(PARTS), dma(PARTS),
            dma(n_row, PARTS), dma(n_row, PARTS), dma(n_row, PARTS),
            dma(2 * steps), dma(2 * steps), dma(steps), dma(steps),
            dma(far), dma(2, n_hi, nm), dma(n_ex), dma(n_ex),
        ],
        compiler_params=pltpu.CompilerParams(
            has_side_effects=True, vmem_limit_bytes=63 * 2**20, **own_barrier
        ),
    )(ld_matrix, factor, diag_values.reshape(width // LANES, LANES))


def solution(mesh):
    in_specs = (P("row", "col"), P(("row", "col"), None), P("col"))
    out_specs = P(("row", "col"), None)
    return jax.shard_map(local, mesh=mesh, in_specs=in_specs, out_specs=out_specs, check_vma=False)
```
